256 devices in a mesh: parts: 2 (over z), node: 8 (over x), local: 16 (over y, core).
Axes of the slice: x: 8, y: 8, z: 2, core: 2. Of those that a mesh axis runs over, the one named last changes fastest.
The devices are a block of a 8x8x16 slice.
Arguments:
- tokens: bfloat16 [2048, 7168], P(('parts', 'node', 'local')), parts along dimension 0, may hold values from -6 to 6
- expert_ids: int32 [2048, 8], P(('parts', 'node', 'local')), parts along dimension 0, may hold values from 0 to 15, as said below
- gate_weights: bfloat16 [2048, 8], P(('parts', 'node', 'local')), parts along dimension 0, may hold values from 0.099609375 to 1
- slots: int32 [2048, 8], P(('parts', 'node', 'local')), parts along dimension 0, may hold values from 0 to 8, as said below
- w_gate: bfloat16 [32, 7168, 2048], P(('parts', 'node'), None, 'local'), parts along dimension 0, may hold values from -0.0625 to 0.0625
- w_up: bfloat16 [32, 7168, 2048], P(('parts', 'node'), None, 'local'), parts along dimension 0, may hold values from -0.0625 to 0.0625
- w_down: bfloat16 [32, 2048, 7168], P(('parts', 'node'), 'local'), parts along dimension 0, may hold values from -0.125 to 0.125
Outputs:
- combined: bfloat16 [2048, 7168], P(('parts', 'node', 'local')), parts along dimension 0
The draws below stay inside these ranges and needn't reach their ends.
There are 2 independent parts, one for each index of `parts`. The reference program is written for one: setup_inputs(seed, part) draws one part's arguments, and reference() takes and returns one part's arrays. A program takes and returns all parts, laid end to end along the dimension named above; each array names one. Nothing has to cross between parts.
Inputs may be any that keep to these rules, and one draw needn't show every extreme that they name: `expert_ids`: each row names 8 different experts, all within at most 4 node groups; expert e belongs to node group e // 2. slots[t, n] is below 8 exactly where some expert of token t belongs to node group n, and equals 8 elsewhere; within each aligned block of 8 rows (the rows of one device) the values below 8 in one column are distinct.
All inputs are finite; a program needn't handle non-finite values.
Results may differ from the reference program's by a relative error of at most 0.019.
Values may be sent and summed in bfloat16 or wider, within the bound.
No kernel may reach another device: no remote copies, remote signals or barrier semaphores. Data moves between devices by JAX's collectives and lax.ppermute only.
A program may use at most 192 MiB of HBM per device.

```python
import math
import jax
import jax.numpy as jnp
from jax import lax

D = 7168
FF = 2048
EXP_NODE = 2
TOP = 8
GROUPS = 4
TOK_DEV = 8
TOKENS = 1024
EXPERTS = 16
N_NODE = 8
N_LOCAL = 16


def routing(key):
    base_key = jax.random.fold_in(key, 7)
    row_keys = jax.random.split(base_key, TOKENS)

    def one_row(row_key):
        first_key, second_key = jax.random.split(row_key)
        chosen_groups = jax.random.permutation(first_key, N_NODE)[:GROUPS]
        picked = jax.random.permutation(second_key, GROUPS * EXP_NODE)[:TOP]
        candidates = (chosen_groups[:, None] * EXP_NODE + jnp.arange(EXP_NODE)[None, :]).reshape(-1)
        return candidates[picked]
    return jax.vmap(one_row)(row_keys).astype(jnp.int32)


def draw_expert_ids(key, part):
    return routing(key)


def draw_slots(key, part):
    chosen = routing(key)
    owners = chosen // EXP_NODE
    reach = jnp.any(owners[:, :, None] == jnp.arange(N_NODE)[None, None, :], axis=1).astype(jnp.int32)
    blocks = reach.reshape(TOKENS // TOK_DEV, TOK_DEV, N_NODE)
    order_key = jax.random.fold_in(key, 11)
    block_keys = jax.random.split(order_key, TOKENS // TOK_DEV * N_NODE)

    def one_order(order_seed):
        return jax.random.permutation(order_seed, TOK_DEV).astype(jnp.int32)
    priority = jax.vmap(one_order)(block_keys).reshape(TOKENS // TOK_DEV, N_NODE, TOK_DEV)
    priority = jnp.transpose(priority, (0, 2, 1))
    scores = priority + (1 - blocks) * TOK_DEV
    ordering = jnp.argsort(scores, axis=1, stable=True)
    ranked = jnp.argsort(ordering, axis=1, stable=True).astype(jnp.int32)
    placed = jnp.where(blocks > 0, ranked, TOK_DEV)
    return placed.reshape(TOKENS, N_NODE).astype(jnp.int32)


def steps_of(key, extent, cuts, least, top_value):
    gain = 1.0
    for position, parts in cuts:
        draws = jax.random.uniform(jax.random.fold_in(jax.random.fold_in(key, 6), position), (parts,), jnp.float32, least / len(cuts), top_value / len(cuts))
        gain = gain * jnp.repeat(jnp.exp(draws), extent[position] // parts).reshape((-1,) + (1,) * (len(extent) - 1 - position))
    return gain


def noise(key, dims, scale, limit, shards=(), held_as=jnp.bfloat16):
    drawn = scale * jax.random.normal(key, dims, jnp.float32)
    if shards:
        drawn = drawn * steps_of(key, dims, shards, -0.22, 0.18)
    return jnp.clip(drawn, -limit, limit).astype(held_as)


def setup_inputs(seed: int = 0, part: int = 0) -> dict:
    arg_keys = jax.random.split(jax.random.key(seed), 8)
    part_splits = jax.random.split(jax.random.fold_in(arg_keys[7], part), 8)
    return {
        "tokens": noise(part_splits[0], (TOKENS, D), 1.0, 6.0, ((0, 128),)),
        "expert_ids": draw_expert_ids(jax.random.fold_in(jax.random.fold_in(arg_keys[7], part), 71), part),
        "gate_weights": jnp.clip(jnp.exp(math.log(1.0) - 2.306499 * jax.random.uniform(part_splits[2], (TOKENS, TOP), jnp.float32) ** steps_of(part_splits[2], (TOKENS, TOP), ((0, 128),), -0.2, 0.2)), 0.099609375, 1.0).astype(jnp.bfloat16),
        "slots": draw_slots(jax.random.fold_in(jax.random.fold_in(arg_keys[7], part), 71), part),
        "w_gate": noise(part_splits[4], (EXPERTS, D, FF), D ** -0.5, 0.0625, ((0, 8), (2, 16))),
        "w_up": noise(part_splits[5], (EXPERTS, D, FF), D ** -0.5, 0.0625, ((0, 8), (2, 16))),
        "w_down": noise(part_splits[6], (EXPERTS, FF, D), FF ** -0.5, 0.125, ((0, 8), (1, 16))),
    }


def reference(tokens, expert_ids, gate_weights, slots, w_gate, w_up, w_down):
    experts_all = EXP_NODE * N_NODE
    matches = (expert_ids[:, :, None] == jnp.arange(experts_all, dtype=jnp.int32)[None, None, :]).astype(jnp.float32)
    token_gates = jnp.sum(gate_weights.astype(jnp.float32)[:, :, None] * matches, axis=1)
    reached = (slots < TOK_DEV).astype(jnp.float32)
    token_gates = token_gates * jnp.repeat(reached, EXP_NODE, axis=1)
    unit_share = FF // N_LOCAL

    def node_term(group):
        summed = jnp.zeros((N_LOCAL, TOKENS, D), jnp.float32)
        for member in range(EXP_NODE):
            expert = (group * EXP_NODE + member).astype(jnp.int32)
            gate_matrix = lax.dynamic_index_in_dim(w_gate, expert, 0, keepdims=False)
            up_matrix = lax.dynamic_index_in_dim(w_up, expert, 0, keepdims=False)
            down_matrix = lax.dynamic_index_in_dim(w_down, expert, 0, keepdims=False)
            gate_value = jnp.dot(tokens, gate_matrix, preferred_element_type=jnp.float32)
            up_value = jnp.dot(tokens, up_matrix, preferred_element_type=jnp.float32)
            hidden = (jax.nn.silu(gate_value) * up_value).astype(jnp.bfloat16)
            hidden_blocks = hidden.reshape(TOKENS, N_LOCAL, unit_share).astype(jnp.float32)
            down_blocks = down_matrix.reshape(N_LOCAL, unit_share, D).astype(jnp.float32)
            shares = jnp.einsum("tlf,lfd->ltd", hidden_blocks, down_blocks, precision=lax.Precision.HIGHEST)
            weight_column = lax.dynamic_index_in_dim(token_gates, expert, 1, keepdims=False)
            summed = summed + weight_column[None, :, None] * shares
        rounded = lax.optimization_barrier(summed.astype(jnp.bfloat16)).astype(jnp.float32)
        return jnp.sum(rounded, axis=0).astype(jnp.bfloat16)

    node_rows = lax.map(node_term, jnp.arange(N_NODE, dtype=jnp.int32))
    return jnp.sum(node_rows.astype(jnp.float32), axis=0).astype(jnp.bfloat16)
```

```python
import jax
import jax.numpy as jnp
from jax import lax
from jax.sharding import Mesh, PartitionSpec as P


PLANE = ("node", "chip", "core")
LANES = 128


def shift_pairs(nodes, chips, cores, first_axis, step):
    pairs = []
    for x in range(nodes):
        for y in range(chips):
            for c in range(cores):
                along_x = (c == 0) == first_axis
                tx, ty = ((x + step) % nodes, y) if along_x else (x, (y + step) % chips)
                pairs.append(((x * chips + y) * cores + c, (tx * chips + ty) * cores + c))
    return pairs


def gates_of(expert_ids, gate_weights, slots, per_node):
    token_count, node_count = slots.shape
    experts_all = node_count * per_node
    matches = (
        expert_ids[:, :, None] == jnp.arange(experts_all, dtype=jnp.int32)[None, None, :]
    ).astype(jnp.float32)
    token_gates = jnp.sum(gate_weights.astype(jnp.float32)[:, :, None] * matches, axis=1)
    reached = (slots < token_count).astype(jnp.float32)
    return token_gates * jnp.repeat(reached, per_node, axis=1)


def build(nodes, chips, cores):
    def move(x, first_axis, step):
        return lax.ppermute(x, PLANE, shift_pairs(nodes, chips, cores, first_axis, step))

    def ring_gather(piece):
        half = piece.shape[0] // 2
        got = {0: piece}
        right = left = piece
        for k in (1, 2, 3):
            right, left = move(right, False, 1), move(left, False, -1)
            got[-k], got[k] = right, left
        got[4] = jnp.concatenate(
            [move(right[:half], False, 1), move(left[half:], False, -1)], axis=0
        )
        return got

    def add(a, b):
        return (a.astype(jnp.float32) + b.astype(jnp.float32)).astype(a.dtype)

    def ring_sum(out):
        half = out[0].shape[0] // 2
        to_left = move(out[4][:half], False, -1)
        to_right = move(out[4][half:], False, 1)
        to_left = jnp.concatenate([add(out[-3][:half], to_left), out[-3][half:]], axis=0)
        to_right = jnp.concatenate([out[3][:half], add(out[3][half:], to_right)], axis=0)
        for k in (2, 1):
            to_left = add(out[-k], move(to_left, False, -1))
            to_right = add(out[k], move(to_right, False, 1))
        total = out[0].astype(jnp.float32) + move(to_left, False, -1).astype(jnp.float32)
        return total + move(to_right, False, 1).astype(jnp.float32)

    def local(tokens, expert_ids, gate_weights, slots, w_gate, w_up, w_down):
        count, width = tokens.shape
        per_node, _, units = w_gate.shape
        swap = [(c, cores - 1 - c) for c in range(cores)]
        pair_gate = lax.ppermute(w_gate, "core", swap)
        pair_up = lax.ppermute(w_up, "core", swap)
        pair_down = lax.ppermute(w_down, "core", swap)

        token_gates = gates_of(expert_ids, gate_weights, slots, per_node).astype(jnp.bfloat16)
        token_gates = jnp.pad(token_gates, ((0, 0), (0, LANES - token_gates.shape[1])))
        own = jnp.concatenate([tokens, token_gates], axis=1)

        near = {0: own}
        for k in (1, -1, 2, -2, 3, -3):
            near[-k] = move(own, True, k)
        near[4] = move(near[-3], True, 1)
        chunks = ((0, -1, 1, -2), (2, -3, 3, 4))

        w_in = jnp.concatenate(
            [w[m] for w in (w_gate, pair_gate, w_up, pair_up) for m in range(per_node)], axis=1
        )
        w_out = jnp.concatenate([w[m] for w in (w_down, pair_down) for m in range(per_node)], axis=0)
        w_in, w_out = lax.optimization_barrier((w_in, w_out))
        hidden_all = w_out.shape[0]
        member = (jnp.arange(hidden_all, dtype=jnp.int32) // units) % per_node
        pick = (
            jnp.arange(LANES, dtype=jnp.int32)[:, None]
            == (lax.axis_index("node") * per_node + member)[None, :]
        ).astype(jnp.bfloat16)

        order = (4, -3, 3, -2, 2, -1, 1, 0)
        total = None
        for offsets in chunks:
            piece = jnp.concatenate([near[d] for d in offsets], axis=0)
            got = ring_gather(piece)
            rows = jnp.concatenate([got[d] for d in order], axis=0)
            gates = jnp.dot(rows[:, width:], pick, preferred_element_type=jnp.float32)
            pre = jnp.dot(rows[:, :width], w_in, preferred_element_type=jnp.float32)
            hidden = gates * (jax.nn.silu(pre[:, :hidden_all]) * pre[:, hidden_all:])
            out = jnp.dot(
                hidden.astype(jnp.bfloat16), w_out, preferred_element_type=jnp.float32
            ).astype(jnp.bfloat16)
            size = piece.shape[0]
            parts = {d: out[i * size : (i + 1) * size] for i, d in enumerate(order)}
            sums = ring_sum(parts)
            rounded = sums.astype(jnp.bfloat16)
            for i, d in enumerate(offsets):
                if d == 0:
                    term = sums[i * count : (i + 1) * count]
                else:
                    term = move(rounded[i * count : (i + 1) * count], True, d).astype(jnp.float32)
                total = term if total is None else total + term
        return total.astype(jnp.bfloat16)

    return local


def solution(mesh):
    parts, nodes, shares = mesh.devices.shape
    cores = 2
    chips = shares // cores
    plane = Mesh(
        mesh.devices.reshape(parts, nodes, chips, cores), ("parts", "node", "chip", "core")
    )
    token_spec = P(("parts", "node", "chip", "core"), None)
    in_specs = (
        token_spec,
        token_spec,
        token_spec,
        token_spec,
        P(("parts", "node"), None, ("chip", "core")),
        P(("parts", "node"), None, ("chip", "core")),
        P(("parts", "node"), ("chip", "core"), None),
    )
    return jax.shard_map(
        build(nodes, chips, cores),
        mesh=plane,
        in_specs=in_specs,
        out_specs=token_spec,
        check_vma=False,
    )
```

```python
import functools

import jax
import jax.numpy as jnp
from jax import lax
from jax.experimental import pallas as pl
from jax.experimental.pallas import tpu as pltpu
from jax.sharding import Mesh, PartitionSpec as P


PLANE = ("node", "chip", "core")
LANES = 128


def place(chips, cores, x, y, c):
    return (x * chips + y) * cores + c


def shift_pairs(nodes, chips, cores, ring, step):
    pairs = []
    for x in range(nodes):
        for y in range(chips):
            for c in range(cores):
                along_x = (c == 0) != ring
                tx, ty = ((x + step) % nodes, y) if along_x else (x, (y + step) % chips)
                pairs.append((place(chips, cores, x, y, c), place(chips, cores, tx, ty, c)))
    return pairs


def expert_kernel(pieces, width, top, count, node_ref, *refs):
    x_refs, refs = refs[:pieces], refs[pieces:]
    w_gate, w_up, w_down, p_gate, p_up, p_down = refs[:6]
    out_refs, refs = refs[6 : 6 + pieces], refs[6 + pieces :]
    in_buf, down_buf, acc, hid, in_sems, down_sems = refs
    per_node, _, units = w_gate.shape
    lanes = per_node * units
    block = in_buf.shape[2] // in_sems.shape[1]
    steps = in_sems.shape[1]
    sources = (w_gate, p_gate, w_up, p_up)

    def in_copy(i, k):
        return pltpu.make_async_copy(
            sources[i].at[:, pl.ds(k * block, block)],
            in_buf.at[pl.ds(i * per_node, per_node), 0, pl.ds(k * block, block)],
            in_sems.at[i, k],
        )

    def down_copy(i):
        return pltpu.make_async_copy((w_down, p_down)[i], down_buf.at[i], down_sems.at[i])

    for k in range(steps):
        for i in range(4):
            in_copy(i, k).start()
    for i in range(2):
        down_copy(i).start()

    acc[...] = jnp.zeros_like(acc)

    @pl.loop(0, steps)
    def _(k):
        for i in range(4):
            in_copy(i, k).wait()
        at = pl.ds(pl.multiple_of(k * block, block), block)
        x = jnp.concatenate([r[:, at] for r in x_refs], axis=0)
        for i in range(4):
            w = jnp.concatenate([in_buf[i * per_node + m, 0, at] for m in range(per_node)], axis=1)
            acc[:, i * lanes : (i + 1) * lanes] += jnp.dot(
                x, w, preferred_element_type=jnp.float32
            )

    meta = jnp.concatenate([r[:, width : width + LANES] for r in x_refs], axis=0)
    meta = meta.astype(jnp.float32)
    lane = lax.broadcasted_iota(jnp.int32, meta.shape, 1)
    weights = pltpu.roll(meta, LANES - top, 1)
    node = node_ref[0]
    slot = jnp.sum(jnp.where(lane == 2 * top + node, meta, 0.0), axis=1, keepdims=True)
    reached = jnp.where(slot < count, 1.0, 0.0)
    gates = []
    for m in range(per_node):
        expert = (node * per_node + m).astype(jnp.float32)
        hit = jnp.logical_and(lane < top, meta == expert)
        gates.append(jnp.sum(jnp.where(hit, weights, 0.0), axis=1, keepdims=True) * reached)
    for i in range(2):
        for m in range(per_node):
            at = i * lanes + m * units
            g = acc[:, at : at + units]
            u = acc[:, 2 * lanes + at : 2 * lanes + at + units]
            hid[:, at : at + units] = (gates[m] * (g / (1.0 + jnp.exp(-g)) * u)).astype(hid.dtype)

    for i in range(2):
        down_copy(i).wait()
    rows = out_refs[0].shape[0]
    own = hid[:, :lanes]
    pair = hid[:, lanes:]

    @pl.loop(0, steps)
    def _(k):
        at = pl.ds(pl.multiple_of(k * block, block), block)
        y = jnp.dot(
            own, down_buf[0, :, :, at].reshape(lanes, block), preferred_element_type=jnp.float32
        )
        y += jnp.dot(
            pair, down_buf[1, :, :, at].reshape(lanes, block), preferred_element_type=jnp.float32
        )
        for j, o in enumerate(out_refs):
            o[:, at] = y[j * rows : (j + 1) * rows].astype(o.dtype)


def experts(node, pieces, w_gate, w_up, w_down, p_gate, p_up, p_down, top, count):
    rows = pieces[0].shape[0]
    per_node, width, units = w_gate.shape
    lanes = per_node * units
    steps = 7 if width % (7 * LANES) == 0 else 1
    total = rows * len(pieces)
    vmem = pl.BlockSpec(memory_space=pltpu.VMEM)
    hbm = pl.BlockSpec(memory_space=pltpu.HBM)
    held = [
        pltpu.with_memory_space_constraint(w, pltpu.HBM)
        for w in (w_gate, w_up, w_down, p_gate, p_up, p_down)
    ]
    return pl.pallas_call(
        functools.partial(expert_kernel, len(pieces), width, top, count),
        out_shape=[jax.ShapeDtypeStruct((rows, width), pieces[0].dtype)] * len(pieces),
        in_specs=[pl.BlockSpec(memory_space=pltpu.SMEM)] + [vmem] * len(pieces) + [hbm] * 6,
        out_specs=[vmem] * len(pieces),
        scratch_shapes=[
            pltpu.VMEM((4 * per_node, 1, width, units), w_gate.dtype),
            pltpu.VMEM((2, per_node, units, width), w_down.dtype),
            pltpu.VMEM((total, 4 * lanes), jnp.float32),
            pltpu.VMEM((total, 2 * lanes), w_down.dtype),
            pltpu.SemaphoreType.DMA((4, steps)),
            pltpu.SemaphoreType.DMA((2,)),
        ],
        compiler_params=pltpu.CompilerParams(vmem_limit_bytes=28 * 2**20),
        cost_estimate=pl.CostEstimate(
            flops=2 * total * width * 6 * lanes,
            bytes_accessed=12 * lanes * width * 2 + 4 * total * width,
            transcendentals=total * 2 * lanes,
        ),
        name="experts",
    )(node, *pieces, *held)


def build(nodes, chips, cores):
    reach = nodes // 2

    def ring_move(x, step):
        return lax.ppermute(x, PLANE, shift_pairs(nodes, chips, cores, True, step))

    def line_move(x, step):
        return lax.ppermute(x, PLANE, shift_pairs(nodes, chips, cores, False, step))

    def add(a, b):
        return (a.astype(jnp.float32) + b.astype(jnp.float32)).astype(a.dtype)

    def local(tokens, expert_ids, gate_weights, slots, w_gate, w_up, w_down):
        count, _ = tokens.shape
        top = expert_ids.shape[1]
        node = lax.axis_index("node").astype(jnp.int32).reshape(1)

        meta = jnp.concatenate([a.astype(tokens.dtype) for a in (expert_ids, gate_weights, slots)], 1)
        meta = jnp.pad(meta, ((0, 0), (0, LANES - meta.shape[1])))
        own = jnp.concatenate([tokens, meta], axis=1)

        low, high, across = line_move(own, 1), line_move(own, -1), line_move(own, reach)
        low, high, across = lax.optimization_barrier((low, high, across))
        near = jnp.concatenate([own, low, high, across], axis=0)
        far_low = line_move(jnp.concatenate([own, low], axis=0), 2)
        far_high = line_move(jnp.concatenate([own, high], axis=0), -2)
        far_low, far_high = lax.optimization_barrier((far_low, far_high))
        far = jnp.concatenate([far_low, far_high], axis=0)

        swap = [(c, cores - 1 - c) for c in range(cores)]
        ready, *gate = lax.optimization_barrier((near, w_gate, w_up, w_down))
        weights = (w_gate, w_up, w_down) + tuple(lax.ppermute(w, "core", swap) for w in gate)

        right, left = [ready, far], [ready, far]
        got = [{0: right[0]}, {0: right[1]}]
        for k in range(1, reach + 1):
            for c in range(2):
                if k < reach:
                    pair = ring_move(right[c], 1), ring_move(left[c], -1)
                    right[c], left[c] = lax.optimization_barrier(pair)
                    got[c][-k], got[c][k] = right[c], left[c]
                else:
                    got[c][k] = ring_move(right[c], 1) if c == 0 else ring_move(left[c], -1)

        offsets = [reach] + [s * k for k in range(reach - 1, 0, -1) for s in (-1, 1)] + [0]
        outs = []
        for c in range(2):
            parts = list(experts(node, [got[c][d] for d in offsets], *weights, top, count))
            if c == 0:
                node, parts[-1] = lax.optimization_barrier((node, parts[-1]))
            outs.append(dict(zip(offsets, parts)))

        to_left, to_right, sums = [None, None], [None, None], []
        for k in range(reach, 0, -1):
            for c in range(2):
                out = outs[c]
                if k == reach:
                    moved = ring_move(out[k], -1 if c == 0 else 1)
                    (to_left if c == 0 else to_right)[c] = moved
                else:
                    go_left = out[-k] if to_left[c] is None else add(out[-k], to_left[c])
                    go_right = out[k] if to_right[c] is None else add(out[k], to_right[c])
                    go_left, go_right = lax.optimization_barrier((go_left, go_right))
                    to_left[c], to_right[c] = ring_move(go_left, -1), ring_move(go_right, 1)
        for c in range(2):
            sums.append(add(add(outs[c][0].astype(jnp.float32), to_left[c]), to_right[c]))

        total = sums[0][:count]
        for value, offsets in zip(sums, ((0, -1, 1, reach), (-2, -3, 2, 3))):
            value = value.astype(tokens.dtype)
            for i, d in enumerate(offsets):
                if d:
                    total = total + line_move(value[i * count : (i + 1) * count], d).astype(
                        jnp.float32
                    )
        return total.astype(tokens.dtype)

    return local


def solution(mesh):
    parts, nodes, shares = mesh.devices.shape
    cores = 2
    chips = shares // cores
    plane = Mesh(
        mesh.devices.reshape(parts, nodes, chips, cores), ("parts", "node", "chip", "core")
    )
    token_spec = P(("parts", "node", "chip", "core"), None)
    in_specs = (
        token_spec,
        token_spec,
        token_spec,
        token_spec,
        P(("parts", "node"), None, ("chip", "core")),
        P(("parts", "node"), None, ("chip", "core")),
        P(("parts", "node"), ("chip", "core"), None),
    )
    return jax.shard_map(
        build(nodes, chips, cores),
        mesh=plane,
        in_specs=in_specs,
        out_specs=token_spec,
        check_vma=False,
    )
```

```python
import functools

import jax
import jax.numpy as jnp
from jax import lax
from jax.experimental import pallas as pl
from jax.experimental.pallas import tpu as pltpu
from jax.sharding import Mesh, PartitionSpec as P


PLANE = ("node", "chip", "core")
LANES = 128
VMEM_LIMIT = 16 * 2**20


def place(chips, cores, x, y, c):
    return (x * chips + y) * cores + c


def shift_pairs(nodes, chips, cores, ring, step):
    pairs = []
    for x in range(nodes):
        for y in range(chips):
            for c in range(cores):
                along_x = (c == 0) != ring
                tx, ty = ((x + step) % nodes, y) if along_x else (x, (y + step) % chips)
                pairs.append((place(chips, cores, x, y, c), place(chips, cores, tx, ty, c)))
    return pairs


def expert_kernel(pieces, width, top, count, steps, node_ref, *refs):
    x_refs, refs = refs[:pieces], refs[pieces:]
    w_gate, w_up, w_down, p_gate, p_up, p_down = refs[:6]
    out_refs, (acc, hid) = refs[6 : 6 + pieces], refs[6 + pieces :]
    per_node, _, units = w_gate.shape
    lanes = per_node * units
    block = width // steps
    acc[...] = jnp.zeros_like(acc)

    @pl.loop(0, steps)
    def _(k):
        at = pl.ds(pl.multiple_of(k * block, block), block)
        x = jnp.concatenate([r[:, at] for r in x_refs], axis=0)
        for i, source in enumerate((w_gate, p_gate, w_up, p_up)):
            w = jnp.concatenate([source[m, at] for m in range(per_node)], axis=1)
            acc[:, i * lanes : (i + 1) * lanes] += jnp.dot(
                x, w, preferred_element_type=jnp.float32
            )

    meta = jnp.concatenate([r[:, width : width + LANES] for r in x_refs], axis=0)
    meta = meta.astype(jnp.float32)
    lane = lax.broadcasted_iota(jnp.int32, meta.shape, 1)
    weights = pltpu.roll(meta, LANES - top, 1)
    node = node_ref[0]
    slot = jnp.sum(jnp.where(lane == 2 * top + node, meta, 0.0), axis=1, keepdims=True)
    reached = jnp.where(slot < count, 1.0, 0.0)
    gates = []
    for m in range(per_node):
        expert = (node * per_node + m).astype(jnp.float32)
        hit = jnp.logical_and(lane < top, meta == expert)
        gates.append(jnp.sum(jnp.where(hit, weights, 0.0), axis=1, keepdims=True) * reached)
    for i in range(2):
        for m in range(per_node):
            at = i * lanes + m * units
            g = acc[:, at : at + units]
            u = acc[:, 2 * lanes + at : 2 * lanes + at + units]
            hid[:, at : at + units] = (gates[m] * (g / (1.0 + jnp.exp(-g)) * u)).astype(hid.dtype)

    rows = out_refs[0].shape[0]
    block //= 2

    @pl.loop(0, 2 * steps)
    def _(k):
        at = pl.ds(pl.multiple_of(k * block, block), block)
        y = jnp.dot(
            hid[:, :lanes],
            w_down[:, :, at].reshape(lanes, block),
            preferred_element_type=jnp.float32,
        )
        y += jnp.dot(
            hid[:, lanes:],
            p_down[:, :, at].reshape(lanes, block),
            preferred_element_type=jnp.float32,
        )
        for j, o in enumerate(out_refs):
            o[:, at] = y[j * rows : (j + 1) * rows].astype(o.dtype)


def experts(node, pieces, weights, top, count):
    rows = pieces[0].shape[0]
    per_node, width, units = weights[0].shape
    lanes = per_node * units
    steps = next(n for n in (14, 7, 1) if width % (n * LANES) == 0)
    total = rows * len(pieces)
    vmem = pl.BlockSpec(memory_space=pltpu.VMEM)
    return pl.pallas_call(
        functools.partial(expert_kernel, len(pieces), width, top, count, steps),
        out_shape=[jax.ShapeDtypeStruct((rows, width), pieces[0].dtype)] * len(pieces),
        in_specs=[pl.BlockSpec(memory_space=pltpu.SMEM)] + [vmem] * (len(pieces) + 6),
        out_specs=[vmem] * len(pieces),
        scratch_shapes=[
            pltpu.VMEM((total, 4 * lanes), jnp.float32),
            pltpu.VMEM((total, 2 * lanes), weights[2].dtype),
        ],
        compiler_params=pltpu.CompilerParams(vmem_limit_bytes=VMEM_LIMIT),
        cost_estimate=pl.CostEstimate(
            flops=2 * total * width * 6 * lanes,
            bytes_accessed=4 * total * width,
            transcendentals=total * 2 * lanes,
        ),
        name="experts",
    )(node, *pieces, *weights)


def build(nodes, chips, cores):
    reach = nodes // 2

    def ring_move(x, step):
        return lax.ppermute(x, PLANE, shift_pairs(nodes, chips, cores, True, step))

    def line_move(x, step):
        return lax.ppermute(x, PLANE, shift_pairs(nodes, chips, cores, False, step))

    def add(a, b):
        return (a.astype(jnp.float32) + b.astype(jnp.float32)).astype(a.dtype)

    def local(tokens, expert_ids, gate_weights, slots, w_gate, w_up, w_down):
        count, _ = tokens.shape
        top = expert_ids.shape[1]
        node = lax.axis_index("node").astype(jnp.int32).reshape(1)

        meta = jnp.concatenate([a.astype(tokens.dtype) for a in (expert_ids, gate_weights, slots)], 1)
        meta = jnp.pad(meta, ((0, 0), (0, LANES - meta.shape[1])))
        own = jnp.concatenate([tokens, meta], axis=1)

        near = line_move(own, 1), line_move(own, -1), line_move(own, reach)
        low, high, across = lax.optimization_barrier(near)
        near = jnp.concatenate([own, low, high, across], axis=0)
        far_low = line_move(jnp.concatenate([own, low], axis=0), 2)
        far_high = line_move(jnp.concatenate([own, high], axis=0), -2)
        far = jnp.concatenate(lax.optimization_barrier((far_low, far_high)), axis=0)

        swap = [(c, cores - 1 - c) for c in range(cores)]
        weights = (w_gate, w_up, w_down) + tuple(
            lax.ppermute(w, "core", swap) for w in (w_gate, w_up, w_down)
        )
        weights = [pltpu.with_memory_space_constraint(w, pltpu.VMEM) for w in weights]

        right, left = [near, far], [near, far]
        got = [{0: right[0]}, {0: right[1]}]
        for k in range(1, reach + 1):
            for c in range(2):
                if k < reach:
                    pair = ring_move(right[c], 1), ring_move(left[c], -1)
                    right[c], left[c] = lax.optimization_barrier(pair)
                    got[c][-k], got[c][k] = right[c], left[c]
                else:
                    got[c][k] = ring_move(right[c], 1) if c == 0 else ring_move(left[c], -1)

        outs = [{}, {}]
        for offsets in ((0, -1, 1), (-2, 2), (-3, 3, reach)):
            where = [(c, d) for d in offsets for c in range(2)]
            parts = experts(node, [got[c][d] for c, d in where], weights, top, count)
            for (c, d), part in zip(where, parts):
                outs[c][d] = part

        to_left, to_right, sums = [None, None], [None, None], []
        for k in range(reach, 0, -1):
            for c in range(2):
                out = outs[c]
                if k == reach:
                    moved = ring_move(out[k], -1 if c == 0 else 1)
                    (to_left if c == 0 else to_right)[c] = moved
                else:
                    go_left = out[-k] if to_left[c] is None else add(out[-k], to_left[c])
                    go_right = out[k] if to_right[c] is None else add(out[k], to_right[c])
                    go_left, go_right = lax.optimization_barrier((go_left, go_right))
                    to_left[c], to_right[c] = ring_move(go_left, -1), ring_move(go_right, 1)
        for c in range(2):
            sums.append(add(add(outs[c][0].astype(jnp.float32), to_left[c]), to_right[c]))

        total = sums[0][:count]
        for c, offsets in enumerate(((0, -1, 1, reach), (-2, -3, 2, 3))):
            value = sums[c].astype(tokens.dtype)
            for i, d in enumerate(offsets):
                if d:
                    back = line_move(value[i * count : (i + 1) * count], d)
                    total = total + back.astype(jnp.float32)
        return total.astype(tokens.dtype)

    return local


def solution(mesh):
    parts, nodes, shares = mesh.devices.shape
    cores = 2
    chips = shares // cores
    plane = Mesh(
        mesh.devices.reshape(parts, nodes, chips, cores), ("parts", "node", "chip", "core")
    )
    token_spec = P(("parts", "node", "chip", "core"), None)
    in_specs = (
        token_spec,
        token_spec,
        token_spec,
        token_spec,
        P(("parts", "node"), None, ("chip", "core")),
        P(("parts", "node"), None, ("chip", "core")),
        P(("parts", "node"), ("chip", "core"), None),
    )
    return jax.shard_map(
        build(nodes, chips, cores),
        mesh=plane,
        in_specs=in_specs,
        out_specs=token_spec,
        check_vma=False,
    )
```

```python
import functools

import jax
import jax.numpy as jnp
from jax import lax
from jax.experimental import pallas as pl
from jax.experimental.pallas import tpu as pltpu
from jax.sharding import Mesh, PartitionSpec as P


PLANE = ("node", "chip", "core")
LANES = 128
VMEM_LIMIT = 16 * 2**20


def place(chips, cores, x, y, c):
    return (x * chips + y) * cores + c


def shift_pairs(nodes, chips, cores, ring, step):
    pairs = []
    for x in range(nodes):
        for y in range(chips):
            for c in range(cores):
                along_x = (c == 0) != ring
                tx, ty = ((x + step) % nodes, y) if along_x else (x, (y + step) % chips)
                pairs.append((place(chips, cores, x, y, c), place(chips, cores, tx, ty, c)))
    return pairs


def expert_kernel(pieces, width, top, count, steps, node_ref, *refs):
    x_refs, refs = refs[:pieces], refs[pieces:]
    w_gate, w_up, w_down, p_gate, p_up, p_down = refs[:6]
    out_refs, (acc, hid) = refs[6 : 6 + pieces], refs[6 + pieces :]
    per_node, _, units = w_gate.shape
    lanes = per_node * units
    block = width // steps
    acc[...] = jnp.zeros_like(acc)

    @pl.loop(0, steps)
    def _(k):
        at = pl.ds(pl.multiple_of(k * block, block), block)
        x = jnp.concatenate([r[:, at] for r in x_refs], axis=0)
        for i, source in enumerate((w_gate, p_gate, w_up, p_up)):
            w = jnp.concatenate([source[m, at] for m in range(per_node)], axis=1)
            acc[:, i * lanes : (i + 1) * lanes] += jnp.dot(
                x, w, preferred_element_type=jnp.float32
            )

    meta = jnp.concatenate([r[:, width : width + LANES] for r in x_refs], axis=0)
    meta = meta.astype(jnp.float32)
    lane = lax.broadcasted_iota(jnp.int32, meta.shape, 1)
    weights = pltpu.roll(meta, LANES - top, 1)
    node = node_ref[0]
    slot = jnp.sum(jnp.where(lane == 2 * top + node, meta, 0.0), axis=1, keepdims=True)
    reached = jnp.where(slot < count, 1.0, 0.0)
    gates = []
    for m in range(per_node):
        expert = (node * per_node + m).astype(jnp.float32)
        hit = jnp.logical_and(lane < top, meta == expert)
        gates.append(jnp.sum(jnp.where(hit, weights, 0.0), axis=1, keepdims=True) * reached)
    for i in range(2):
        for m in range(per_node):
            at = i * lanes + m * units
            g = acc[:, at : at + units]
            u = acc[:, 2 * lanes + at : 2 * lanes + at + units]
            hid[:, at : at + units] = (gates[m] * (g / (1.0 + jnp.exp(-g)) * u)).astype(hid.dtype)

    ends = [0]
    for o in out_refs:
        ends.append(ends[-1] + o.shape[0])

    @pl.loop(0, steps)
    def _(k):
        at = pl.ds(pl.multiple_of(k * block, block), block)
        y = jnp.dot(
            hid[:, :lanes],
            w_down[:, :, at].reshape(lanes, block),
            preferred_element_type=jnp.float32,
        )
        y += jnp.dot(
            hid[:, lanes:],
            p_down[:, :, at].reshape(lanes, block),
            preferred_element_type=jnp.float32,
        )
        for j, o in enumerate(out_refs):
            o[:, at] = y[ends[j] : ends[j + 1]].astype(o.dtype)


def experts(node, pieces, weights, top, count):
    per_node, width, units = weights[0].shape
    lanes = per_node * units
    steps = next(n for n in (4, 7, 1) if width % (n * LANES) == 0)
    total = sum(p.shape[0] for p in pieces)
    vmem = pl.BlockSpec(memory_space=pltpu.VMEM)
    return pl.pallas_call(
        functools.partial(expert_kernel, len(pieces), width, top, count, steps),
        out_shape=[jax.ShapeDtypeStruct((p.shape[0], width), p.dtype) for p in pieces],
        in_specs=[pl.BlockSpec(memory_space=pltpu.SMEM)] + [vmem] * (len(pieces) + 6),
        out_specs=[vmem] * len(pieces),
        scratch_shapes=[
            pltpu.VMEM((total, 4 * lanes), jnp.float32),
            pltpu.VMEM((total, 2 * lanes), weights[2].dtype),
        ],
        compiler_params=pltpu.CompilerParams(vmem_limit_bytes=VMEM_LIMIT),
        cost_estimate=pl.CostEstimate(
            flops=2 * total * width * 6 * lanes,
            bytes_accessed=4 * total * width,
            transcendentals=total * 2 * lanes,
        ),
        name="experts",
    )(node, *pieces, *weights)


def build(nodes, chips, cores):
    reach = nodes // 2

    def ring_move(x, step):
        return lax.ppermute(x, PLANE, shift_pairs(nodes, chips, cores, True, step))

    def line_move(x, step):
        return lax.ppermute(x, PLANE, shift_pairs(nodes, chips, cores, False, step))

    def add(a, b):
        return (a.astype(jnp.float32) + b.astype(jnp.float32)).astype(a.dtype)

    def local(tokens, expert_ids, gate_weights, slots, w_gate, w_up, w_down):
        count, _ = tokens.shape
        top = expert_ids.shape[1]
        node = lax.axis_index("node").astype(jnp.int32).reshape(1)

        meta = jnp.concatenate([a.astype(tokens.dtype) for a in (expert_ids, gate_weights, slots)], 1)
        meta = jnp.pad(meta, ((0, 0), (0, LANES - meta.shape[1])))
        own = jnp.concatenate([tokens, meta], axis=1)

        low, high = lax.optimization_barrier((line_move(own, 1), line_move(own, -1)))
        near = jnp.concatenate([low, own, high], axis=0)
        far_low = line_move(near, reach - 1)
        far_high = line_move(near[count:], 2 - reach)
        far = jnp.concatenate(lax.optimization_barrier((far_low, far_high)), axis=0)

        swap = [(c, cores - 1 - c) for c in range(cores)]
        pair = [lax.ppermute(w, "core", swap) for w in (w_gate, w_up, w_down)]
        weights = [
            pltpu.with_memory_space_constraint(w, pltpu.VMEM)
            for w in (w_gate, w_up, w_down, *pair)
        ]

        right, left = [near, far], [near, far]
        got = [{0: right[0]}, {0: right[1]}]
        for k in range(1, reach + 1):
            for c in range(2):
                if k < reach:
                    pair = ring_move(right[c], 1), ring_move(left[c], -1)
                    right[c], left[c] = lax.optimization_barrier(pair)
                    got[c][-k], got[c][k] = right[c], left[c]
                else:
                    got[c][k] = ring_move(right[c], 1) if c == 0 else ring_move(left[c], -1)

        outs = [{}, {}]
        for offsets in ((0, -1, 1), (-2, 2), (-3, 3, reach)):
            where = [(c, d) for d in offsets for c in range(2)]
            parts = experts(node, [got[c][d] for c, d in where], weights, top, count)
            for (c, d), part in zip(where, parts):
                outs[c][d] = part

        to_left, to_right, sums = [None, None], [None, None], []
        for k in range(reach, 0, -1):
            for c in (1, 0):
                out = outs[c]
                if k == reach:
                    moved = ring_move(out[k], -1 if c == 0 else 1)
                    (to_left if c == 0 else to_right)[c] = moved
                else:
                    go_left = out[-k] if to_left[c] is None else add(out[-k], to_left[c])
                    go_right = out[k] if to_right[c] is None else add(out[k], to_right[c])
                    go_left, go_right = lax.optimization_barrier((go_left, go_right))
                    to_left[c], to_right[c] = ring_move(go_left, -1), ring_move(go_right, 1)
        for c in range(2):
            value = add(add(outs[c][0].astype(jnp.float32), to_left[c]), to_right[c])
            sums.append(value if c == 0 else value.astype(tokens.dtype))

        near, far = sums
        triple = line_move(far[: 3 * count], 1 - reach)
        double = line_move(far[3 * count :], reach - 2)
        near = near + triple.astype(jnp.float32)
        double = double.astype(jnp.float32)
        total = near[count : 2 * count] + double[:count]
        low = near[:count].astype(tokens.dtype)
        high = (near[2 * count :] + double[count:]).astype(tokens.dtype)
        low, high = line_move(low, -1), line_move(high, 1)
        total = total + low.astype(jnp.float32) + high.astype(jnp.float32)
        return total.astype(tokens.dtype)

    return local


def solution(mesh):
    parts, nodes, shares = mesh.devices.shape
    cores = 2
    chips = shares // cores
    plane = Mesh(
        mesh.devices.reshape(parts, nodes, chips, cores), ("parts", "node", "chip", "core")
    )
    token_spec = P(("parts", "node", "chip", "core"), None)
    in_specs = (
        token_spec,
        token_spec,
        token_spec,
        token_spec,
        P(("parts", "node"), None, ("chip", "core")),
        P(("parts", "node"), None, ("chip", "core")),
        P(("parts", "node"), ("chip", "core"), None),
    )
    return jax.shard_map(
        build(nodes, chips, cores),
        mesh=plane,
        in_specs=in_specs,
        out_specs=token_spec,
        check_vma=False,
    )
```

```python
import functools

import jax
import jax.numpy as jnp
from jax import lax
from jax.experimental import pallas as pl
from jax.experimental.pallas import tpu as pltpu
from jax.sharding import Mesh, PartitionSpec as P


PLANE = ("node", "chip", "core")
LANES = 128
VMEM_LIMIT = 20 * 2**20


def place(chips, cores, x, y, c):
    return (x * chips + y) * cores + c


def shift_pairs(nodes, chips, cores, ring, step):
    pairs = []
    for x in range(nodes):
        for y in range(chips):
            for c in range(cores):
                along_x = (c == 0) != ring
                tx, ty = ((x + step) % nodes, y) if along_x else (x, (y + step) % chips)
                pairs.append((place(chips, cores, x, y, c), place(chips, cores, tx, ty, c)))
    return pairs


def expert_kernel(pieces, width, top, count, steps, steps_out, node_ref, *refs):
    x_refs, refs = refs[:pieces], refs[pieces:]
    w_gate, w_up, p_gate, p_up, w_down, p_down = refs[:6]
    out_refs, (acc, hid, *held, sems) = refs[6 : 6 + pieces], refs[6 + pieces :]
    per_node, _, units = w_gate.shape
    lanes = per_node * units
    block = width // steps
    copies = [
        pltpu.make_async_copy(source, buf, sems.at[i])
        for i, (source, buf) in enumerate(zip((p_gate, p_up, w_down, p_down), held))
    ]
    for copy in copies:
        copy.start()
    acc[...] = jnp.zeros_like(acc)

    def multiply_in(side, sources):
        @pl.loop(0, steps)
        def _(k):
            at = pl.ds(pl.multiple_of(k * block, block), block)
            x = jnp.concatenate([r[:, at] for r in x_refs], axis=0)
            for i, source in enumerate(sources):
                to = (2 * i + side) * lanes
                w = jnp.concatenate([source[m, at] for m in range(per_node)], axis=1)
                acc[:, to : to + lanes] += jnp.dot(x, w, preferred_element_type=jnp.float32)

    multiply_in(0, (w_gate, w_up))
    copies[0].wait()
    copies[1].wait()
    multiply_in(1, held[:2])

    meta = jnp.concatenate([r[:, width : width + LANES] for r in x_refs], axis=0)
    meta = meta.astype(jnp.float32)
    lane = lax.broadcasted_iota(jnp.int32, meta.shape, 1)
    weights = pltpu.roll(meta, LANES - top, 1)
    node = node_ref[0]
    slot = jnp.sum(jnp.where(lane == 2 * top + node, meta, 0.0), axis=1, keepdims=True)
    reached = jnp.where(slot < count, 1.0, 0.0)
    gates = []
    for m in range(per_node):
        expert = (node * per_node + m).astype(jnp.float32)
        hit = jnp.logical_and(lane < top, meta == expert)
        gates.append(jnp.sum(jnp.where(hit, weights, 0.0), axis=1, keepdims=True) * reached)
    for i in range(2):
        for m in range(per_node):
            at = i * lanes + m * units
            g = acc[:, at : at + units]
            u = acc[:, 2 * lanes + at : 2 * lanes + at + units]
            hid[:, at : at + units] = (gates[m] * (g / (1.0 + jnp.exp(-g)) * u)).astype(hid.dtype)

    copies[2].wait()
    copies[3].wait()
    ends = [0]
    for o in out_refs:
        ends.append(ends[-1] + o.shape[0])

    block = width // steps_out

    @pl.loop(0, steps_out)
    def _(k):
        at = pl.ds(pl.multiple_of(k * block, block), block)
        y = jnp.dot(
            hid[:, :lanes],
            held[2][:, :, at].reshape(lanes, block),
            preferred_element_type=jnp.float32,
        )
        y += jnp.dot(
            hid[:, lanes:],
            held[3][:, :, at].reshape(lanes, block),
            preferred_element_type=jnp.float32,
        )
        for j, o in enumerate(out_refs):
            o[:, at] = y[ends[j] : ends[j + 1]].astype(o.dtype)


def experts(node, pieces, weights, top, count):
    per_node, width, units = weights[0].shape
    lanes = per_node * units
    steps = next(n for n in (4, 7, 1) if width % (n * LANES) == 0)
    steps_out = next(n for n in (7, 4, 1) if width % (n * LANES) == 0)
    total = sum(p.shape[0] for p in pieces)
    vmem = pl.BlockSpec(memory_space=pltpu.VMEM)
    hbm = pl.BlockSpec(memory_space=pltpu.HBM)
    return pl.pallas_call(
        functools.partial(expert_kernel, len(pieces), width, top, count, steps, steps_out),
        out_shape=[jax.ShapeDtypeStruct((p.shape[0], width), p.dtype) for p in pieces],
        in_specs=[pl.BlockSpec(memory_space=pltpu.SMEM)] + [vmem] * (len(pieces) + 2) + [hbm] * 4,
        out_specs=[vmem] * len(pieces),
        scratch_shapes=[
            pltpu.VMEM((total, 4 * lanes), jnp.float32),
            pltpu.VMEM((total, 2 * lanes), weights[0].dtype),
            *[pltpu.VMEM(w.shape, w.dtype) for w in weights[2:]],
            pltpu.SemaphoreType.DMA((4,)),
        ],
        compiler_params=pltpu.CompilerParams(vmem_limit_bytes=VMEM_LIMIT),
        cost_estimate=pl.CostEstimate(
            flops=2 * total * width * 6 * lanes,
            bytes_accessed=4 * total * width,
            transcendentals=total * 2 * lanes,
        ),
        name="experts",
    )(node, *pieces, *weights)


def build(nodes, chips, cores):
    reach = nodes // 2

    def ring_move(x, step):
        return lax.ppermute(x, PLANE, shift_pairs(nodes, chips, cores, True, step))

    def line_move(x, step):
        return lax.ppermute(x, PLANE, shift_pairs(nodes, chips, cores, False, step))

    def add(a, b):
        return (a.astype(jnp.float32) + b.astype(jnp.float32)).astype(a.dtype)

    def local(tokens, expert_ids, gate_weights, slots, w_gate, w_up, w_down):
        count, _ = tokens.shape
        top = expert_ids.shape[1]
        node = lax.axis_index("node").astype(jnp.int32).reshape(1)

        meta = jnp.concatenate([a.astype(tokens.dtype) for a in (expert_ids, gate_weights, slots)], 1)
        meta = jnp.pad(meta, ((0, 0), (0, LANES - meta.shape[1])))
        own = jnp.concatenate([tokens, meta], axis=1)

        low, high = lax.optimization_barrier((line_move(own, 1), line_move(own, -1)))
        near = jnp.concatenate([low, own, high], axis=0)
        far_low = line_move(near, reach - 1)
        far_high = line_move(near[count:], 2 - reach)
        far = jnp.concatenate(lax.optimization_barrier((far_low, far_high)), axis=0)

        swap = [(c, cores - 1 - c) for c in range(cores)]
        pair = [lax.ppermute(w, "core", swap) for w in (w_gate, w_up, w_down)]
        weights = [
            pltpu.with_memory_space_constraint(w, pltpu.VMEM) for w in (w_gate, w_up)
        ] + [
            pltpu.with_memory_space_constraint(w, pltpu.HBM) for w in (*pair[:2], w_down, pair[2])
        ]

        right, left = [near, far], [near, far]
        got = [{0: right[0]}, {0: right[1]}]
        for k in range(1, reach + 1):
            for c in range(2):
                if k < reach:
                    pair = ring_move(right[c], 1), ring_move(left[c], -1)
                    right[c], left[c] = lax.optimization_barrier(pair)
                    got[c][-k], got[c][k] = right[c], left[c]
                else:
                    got[c][k] = ring_move(right[c], 1) if c == 0 else ring_move(left[c], -1)

        outs = [{}, {}]
        for offsets in ((0, -1, 1), (-2, 2), (-3, 3, reach)):
            where = [(c, d) for d in offsets for c in range(2)]
            parts = experts(node, [got[c][d] for c, d in where], weights, top, count)
            for (c, d), part in zip(where, parts):
                outs[c][d] = part

        to_left, to_right, sums = [None, None], [None, None], []
        for k in range(reach, 0, -1):
            for c in (1, 0):
                out = outs[c]
                if k == reach:
                    moved = ring_move(out[k], -1 if c == 0 else 1)
                    (to_left if c == 0 else to_right)[c] = moved
                else:
                    go_left = out[-k] if to_left[c] is None else add(out[-k], to_left[c])
                    go_right = out[k] if to_right[c] is None else add(out[k], to_right[c])
                    go_left, go_right = lax.optimization_barrier((go_left, go_right))
                    to_left[c], to_right[c] = ring_move(go_left, -1), ring_move(go_right, 1)
        for c in range(2):
            value = add(add(outs[c][0].astype(jnp.float32), to_left[c]), to_right[c])
            sums.append(value if c == 0 else value.astype(tokens.dtype))

        near, far = sums
        triple = line_move(far[: 3 * count], 1 - reach)
        double = line_move(far[3 * count :], reach - 2)
        near = near + triple.astype(jnp.float32)
        double = double.astype(jnp.float32)
        total = near[count : 2 * count] + double[:count]
        low = near[:count].astype(tokens.dtype)
        high = (near[2 * count :] + double[count:]).astype(tokens.dtype)
        low, high = line_move(low, -1), line_move(high, 1)
        total = total + low.astype(jnp.float32) + high.astype(jnp.float32)
        return total.astype(tokens.dtype)

    return local


def solution(mesh):
    parts, nodes, shares = mesh.devices.shape
    cores = 2
    chips = shares // cores
    plane = Mesh(
        mesh.devices.reshape(parts, nodes, chips, cores), ("parts", "node", "chip", "core")
    )
    token_spec = P(("parts", "node", "chip", "core"), None)
    in_specs = (
        token_spec,
        token_spec,
        token_spec,
        token_spec,
        P(("parts", "node"), None, ("chip", "core")),
        P(("parts", "node"), None, ("chip", "core")),
        P(("parts", "node"), ("chip", "core"), None),
    )
    return jax.shard_map(
        build(nodes, chips, cores),
        mesh=plane,
        in_specs=in_specs,
        out_specs=token_spec,
        check_vma=False,
    )
```

```python
import functools

import jax
import jax.numpy as jnp
from jax import lax
from jax.experimental import pallas as pl
from jax.experimental.pallas import tpu as pltpu
from jax.sharding import Mesh, PartitionSpec as P


PLANE = ("node", "chip", "core")
LANES = 128
VMEM_LIMIT = 20 * 2**20


def place(chips, cores, x, y, c):
    return (x * chips + y) * cores + c


def shift_pairs(nodes, chips, cores, ring, step):
    pairs = []
    for x in range(nodes):
        for y in range(chips):
            for c in range(cores):
                along_x = (c == 0) != ring
                tx, ty = ((x + step) % nodes, y) if along_x else (x, (y + step) % chips)
                pairs.append((place(chips, cores, x, y, c), place(chips, cores, tx, ty, c)))
    return pairs


def expert_kernel(pieces, width, top, first, count, steps, steps_out, node_ref, *refs):
    x_refs, refs = refs[:pieces], refs[pieces:]
    w_gate, w_up, p_gate, p_up, w_down, p_down = refs[:6]
    out_refs, (acc, hid, *held, sems) = refs[6 : 6 + pieces], refs[6 + pieces :]
    per_node, _, units = w_gate.shape
    lanes = per_node * units
    block = width // steps
    copies = [
        pltpu.make_async_copy(source, buf, sems.at[i])
        for i, (source, buf) in enumerate(zip((p_gate, p_up, w_down, p_down), held))
    ]
    for copy in copies:
        copy.start()
    acc[...] = jnp.zeros_like(acc)

    def multiply_in(side, sources):
        @pl.loop(0, steps)
        def _(k):
            at = pl.ds(pl.multiple_of(k * block, block), block)
            x = jnp.concatenate([r[:, at] for r in x_refs], axis=0)
            for i, source in enumerate(sources):
                to = (2 * i + side) * lanes
                w = jnp.concatenate([source[m, at] for m in range(per_node)], axis=1)
                acc[:, to : to + lanes] += jnp.dot(x, w, preferred_element_type=jnp.float32)

    multiply_in(0, (w_gate, w_up))
    copies[0].wait()
    copies[1].wait()
    multiply_in(1, held[:2])

    meta = jnp.concatenate([r[:, width : width + LANES] for r in x_refs], axis=0)
    meta = meta.astype(jnp.float32)
    lane = lax.broadcasted_iota(jnp.int32, meta.shape, 1)
    weights = pltpu.roll(meta, LANES - first, 1)
    node = node_ref[0]
    slot = jnp.sum(jnp.where(lane == top + node, meta, 0.0), axis=1, keepdims=True)
    reached = jnp.where(slot < count, 1.0, 0.0)
    gates = []
    for m in range(per_node):
        expert = (node * per_node + m).astype(jnp.float32)
        hit = jnp.logical_and(lane < top, meta == expert)
        gates.append(jnp.sum(jnp.where(hit, weights, 0.0), axis=1, keepdims=True) * reached)
    for i in range(2):
        for m in range(per_node):
            at = i * lanes + m * units
            g = acc[:, at : at + units]
            u = acc[:, 2 * lanes + at : 2 * lanes + at + units]
            hid[:, at : at + units] = (gates[m] * (g / (1.0 + jnp.exp(-g)) * u)).astype(hid.dtype)

    copies[2].wait()
    copies[3].wait()
    ends = [0]
    for o in out_refs:
        ends.append(ends[-1] + o.shape[0])

    block = width // steps_out

    @pl.loop(0, steps_out)
    def _(k):
        at = pl.ds(pl.multiple_of(k * block, block), block)
        y = jnp.dot(
            hid[:, :lanes],
            held[2][:, :, at].reshape(lanes, block),
            preferred_element_type=jnp.float32,
        )
        y += jnp.dot(
            hid[:, lanes:],
            held[3][:, :, at].reshape(lanes, block),
            preferred_element_type=jnp.float32,
        )
        for j, o in enumerate(out_refs):
            o[:, at] = y[ends[j] : ends[j + 1]].astype(o.dtype)


def experts(node, pieces, weights, top, first, count):
    per_node, width, units = weights[0].shape
    lanes = per_node * units
    steps = next(n for n in (4, 7, 1) if width % (n * LANES) == 0)
    steps_out = next(n for n in (7, 4, 1) if width % (n * LANES) == 0)
    total = sum(p.shape[0] for p in pieces)
    vmem = pl.BlockSpec(memory_space=pltpu.VMEM)
    hbm = pl.BlockSpec(memory_space=pltpu.HBM)
    return pl.pallas_call(
        functools.partial(expert_kernel, len(pieces), width, top, first, count, steps, steps_out),
        out_shape=[jax.ShapeDtypeStruct((p.shape[0], width), p.dtype) for p in pieces],
        in_specs=[pl.BlockSpec(memory_space=pltpu.SMEM)] + [vmem] * (len(pieces) + 2) + [hbm] * 4,
        out_specs=[vmem] * len(pieces),
        scratch_shapes=[
            pltpu.VMEM((total, 4 * lanes), jnp.float32),
            pltpu.VMEM((total, 2 * lanes), weights[0].dtype),
            *[pltpu.VMEM(w.shape, w.dtype) for w in weights[2:]],
            pltpu.SemaphoreType.DMA((4,)),
        ],
        compiler_params=pltpu.CompilerParams(vmem_limit_bytes=VMEM_LIMIT),
        cost_estimate=pl.CostEstimate(
            flops=2 * total * width * 6 * lanes,
            bytes_accessed=4 * total * width,
            transcendentals=total * 2 * lanes,
        ),
        name="experts",
    )(node, *pieces, *weights)


def build(nodes, chips, cores):
    reach = nodes // 2

    def ring_move(x, step):
        return lax.ppermute(x, PLANE, shift_pairs(nodes, chips, cores, True, step))

    def line_move(x, step):
        return lax.ppermute(x, PLANE, shift_pairs(nodes, chips, cores, False, step))

    def add(a, b):
        return (a.astype(jnp.float32) + b.astype(jnp.float32)).astype(a.dtype)

    def local(tokens, expert_ids, gate_weights, slots, w_gate, w_up, w_down):
        count, _ = tokens.shape
        top = expert_ids.shape[1]
        node = lax.axis_index("node").astype(jnp.int32).reshape(1)

        marks = jnp.concatenate([expert_ids, slots], axis=1).astype(tokens.dtype)
        meta = jnp.concatenate([marks, gate_weights], axis=1)
        meta = jnp.pad(meta, ((0, 0), (0, LANES - meta.shape[1])))
        own = jnp.concatenate([tokens, meta], axis=1)

        low, high = lax.optimization_barrier((line_move(own, 1), line_move(own, -1)))
        near = jnp.concatenate([low, own, high], axis=0)
        far_low = line_move(near, reach - 1)
        far_high = line_move(near[count:], 2 - reach)
        far = jnp.concatenate(lax.optimization_barrier((far_low, far_high)), axis=0)

        swap = [(c, cores - 1 - c) for c in range(cores)]
        pair = [lax.ppermute(w, "core", swap) for w in (w_gate, w_up, w_down)]
        weights = [
            pltpu.with_memory_space_constraint(w, pltpu.VMEM) for w in (w_gate, w_up)
        ] + [
            pltpu.with_memory_space_constraint(w, pltpu.HBM) for w in (*pair[:2], w_down, pair[2])
        ]

        right, left = [near, far], [near, far]
        got = [{0: right[0]}, {0: right[1]}]
        for k in range(1, reach + 1):
            for c in range(2):
                if k < reach:
                    pair = ring_move(right[c], 1), ring_move(left[c], -1)
                    right[c], left[c] = lax.optimization_barrier(pair)
                    got[c][-k], got[c][k] = right[c], left[c]
                else:
                    got[c][k] = ring_move(right[c], 1) if c == 0 else ring_move(left[c], -1)

        outs = [{}, {}]
        for offsets in ((0, -1, 1), (-2, 2, -3, 3, reach)):
            where = [(c, d) for d in offsets for c in range(2)]
            parts = experts(node, [got[c][d] for c, d in where], weights, top, marks.shape[1], count)
            for (c, d), part in zip(where, parts):
                outs[c][d] = part

        to_left, to_right, sums = [None, None], [None, None], []
        for k in range(reach, 0, -1):
            for c in (1, 0):
                out = outs[c]
                if k == reach:
                    moved = ring_move(out[k], -1 if c == 0 else 1)
                    (to_left if c == 0 else to_right)[c] = moved
                else:
                    go_left = out[-k] if to_left[c] is None else add(out[-k], to_left[c])
                    go_right = out[k] if to_right[c] is None else add(out[k], to_right[c])
                    go_left, go_right = lax.optimization_barrier((go_left, go_right))
                    to_left[c], to_right[c] = ring_move(go_left, -1), ring_move(go_right, 1)
        for c in range(2):
            value = add(add(outs[c][0].astype(jnp.float32), to_left[c]), to_right[c])
            sums.append(value if c == 0 else value.astype(tokens.dtype))

        near, far = sums
        triple = line_move(far[: 3 * count], 1 - reach)
        double = line_move(far[3 * count :], reach - 2)
        near = near + triple.astype(jnp.float32)
        double = double.astype(jnp.float32)
        total = near[count : 2 * count] + double[:count]
        low = near[:count].astype(tokens.dtype)
        high = (near[2 * count :] + double[count:]).astype(tokens.dtype)
        low, high = line_move(low, -1), line_move(high, 1)
        total = total + low.astype(jnp.float32) + high.astype(jnp.float32)
        return total.astype(tokens.dtype)

    return local


def solution(mesh):
    parts, nodes, shares = mesh.devices.shape
    cores = 2
    chips = shares // cores
    plane = Mesh(
        mesh.devices.reshape(parts, nodes, chips, cores), ("parts", "node", "chip", "core")
    )
    token_spec = P(("parts", "node", "chip", "core"), None)
    in_specs = (
        token_spec,
        token_spec,
        token_spec,
        token_spec,
        P(("parts", "node"), None, ("chip", "core")),
        P(("parts", "node"), None, ("chip", "core")),
        P(("parts", "node"), ("chip", "core"), None),
    )
    return jax.shard_map(
        build(nodes, chips, cores),
        mesh=plane,
        in_specs=in_specs,
        out_specs=token_spec,
        check_vma=False,
    )
```
